32 devices in a mesh: dp: 8 (over z, core), tensor: 4 (over y, x).
Axes of the slice: x: 2, y: 2, z: 4, core: 2. Of those that a mesh axis runs over, the one named last changes fastest.
Arguments:
- prompt_ids: int32 [4096], P(('dp', 'tensor')), may hold values from 0 to 128255
- prompt_lengths: int32 [8], replicated, may hold values from 1 to 512, as said below
- embed_table: bfloat16 [4096, 128256], P(('dp', 'tensor')), may hold values from -4 to 4
- norm_gain: float32 [4096], replicated, may hold values from 0.5 to 1.5
- w_query: bfloat16 [4096, 4096], P('dp', 'tensor'), may hold values from -3 to 3
- w_key: bfloat16 [4096, 1024], P('dp', 'tensor'), may hold values from -1 to 1
- w_value: bfloat16 [4096, 1024], P('dp', 'tensor'), may hold values from -0.09375 to 0.09375
- w_out: bfloat16 [4096, 4096], P('tensor', 'dp'), may hold values from -0.09375 to 0.09375
Outputs:
- hidden: bfloat16 [4096, 4096], P(('dp', 'tensor'))
- kv_cache: bfloat16 [32, 2, 512, 256], P(('dp', 'tensor'))
The draws below stay inside these ranges and needn't reach their ends.
Inputs may be any that keep to these rules, and one draw needn't show every extreme that they name: `prompt_lengths`: each group's prompt has 1 to 512 live tokens, and some group's has 512.
All inputs are finite; a program needn't handle non-finite values.
Results may differ from the reference program's by a relative error of at most 0.0095.
Values may be sent and summed in bfloat16 or wider, within the bound.
A program may use at most 192 MiB of HBM per device.

```python
import math
import jax
import jax.numpy as jnp
import numpy as np
from jax import lax

D = 4096
HEADS = 32
KVH = 8
HD = 128
VOCAB = 128256
TPG = 4
PROMPT = 512
GROUPS = 8
TOKENS = 4096
N_TENSOR = 4


def draw_prompt_lengths(key, part):
    base = jax.random.randint(jax.random.fold_in(key, 11), (GROUPS,), 1, PROMPT + 1)
    chosen = jax.random.randint(jax.random.fold_in(key, 12), (), 0, GROUPS)
    return jnp.where(jnp.arange(GROUPS) == chosen, PROMPT, base).astype(jnp.int32)


def draw_embed_table(key, part):
    base = jnp.clip(jax.random.normal(jax.random.fold_in(key, 21), (D, VOCAB), jnp.float32), -6.0, 6.0)
    return jnp.clip(0.2 * base, -4.0, 4.0).astype(jnp.bfloat16)


def shared_keys(key):
    base = jax.random.normal(jax.random.fold_in(key, 31), (D, KVH * HD), jnp.float32)
    return jnp.clip(base, -6.0, 6.0) * D ** (-0.5)


def draw_w_key(key, part):
    return jnp.clip(shared_keys(key), -1.0, 1.0).astype(jnp.bfloat16)


def draw_w_query(key, part):
    own = jnp.clip(jax.random.normal(jax.random.fold_in(key, 32), (D, D), jnp.float32), -6.0, 6.0) * D ** (-0.5)
    return jnp.clip(own, -3.0, 3.0).astype(jnp.bfloat16)


def set_ends(values, own_key, smallest, top_value):
    longest = values.shape.index(max(values.shape))
    spots = []
    for shift in (0, 1):
        where = [jax.random.randint(jax.random.fold_in(own_key, axis), (), 0, length) for axis, length in enumerate(values.shape)]
        where[longest] = (where[longest] + shift) % values.shape[longest]
        spots.append(tuple(where))
    return values.at[spots[0]].set(smallest).at[spots[1]].set(top_value)


def level_of(stream_key, shape, pieces, least, top_value):
    gain, own = 1.0, jax.random.fold_in(stream_key, 6)
    for dim, blocks in pieces:
        heights = jnp.exp(jax.random.uniform(jax.random.fold_in(own, dim), (blocks,), jnp.float32, least / len(pieces), top_value / len(pieces)))
        gain = gain * jnp.repeat(heights, shape[dim] // blocks).reshape([-1 if axis == dim else 1 for axis in range(len(shape))])
    return gain


def skewed_wide(stream_key, extent, number_of, slope):
    portions = [min(1 << octave, number_of + 1 - (1 << octave)) * (1 << 20) // math.isqrt((1 << octave) ** slope) + 1 for octave in range((number_of + 1).bit_length()) if 1 << octave <= number_of]
    width = 1 + sum(portions) // (1 << 30)
    grid = np.cumsum(np.array([max(1, weight // width) for weight in portions]))
    lot = jax.random.randint(jax.random.fold_in(stream_key, 1), extent, 0, int(grid[len(portions) - 1]))
    start = jnp.left_shift(1, jnp.searchsorted(jnp.asarray(grid, jnp.int32), lot, side="right").astype(jnp.int32))
    rank = start - 1 + jax.random.randint(jax.random.fold_in(stream_key, 4), extent, 0, 1 << 30) % jnp.minimum(start, number_of + 1 - start)
    return jax.random.permutation(jax.random.fold_in(stream_key, 2), number_of)[rank].astype(jnp.int32)


def scatter_about(stream_key, shape, deviation, bound, split=(), kind=jnp.bfloat16):
    entries = jax.random.normal(stream_key, shape, jnp.float32) * deviation
    if len(split) > 0:
        entries = level_of(stream_key, shape, split, -0.22, 0.18) * entries
    return jnp.clip(entries, min=-bound, max=bound).astype(kind)


def setup_inputs(seed: int = 0) -> dict:
    arg_keys = jax.random.split(jax.random.key(seed), 9)
    return {
        "prompt_ids": set_ends(skewed_wide(arg_keys[0], (TOKENS,), VOCAB, 2), jax.random.fold_in(arg_keys[0], 3), 0, VOCAB - 1).astype(jnp.int32),
        "prompt_lengths": draw_prompt_lengths(jax.random.fold_in(arg_keys[8], 71), 0),
        "embed_table": draw_embed_table(jax.random.fold_in(arg_keys[8], 71), 0),
        "norm_gain": jnp.clip(1.0 + 0.1 * jax.random.normal(arg_keys[3], (D,), jnp.float32), 0.5, 1.5),
        "w_query": draw_w_query(jax.random.fold_in(arg_keys[8], 71), 0),
        "w_key": draw_w_key(jax.random.fold_in(arg_keys[8], 71), 0),
        "w_value": scatter_about(arg_keys[6], (D, KVH * HD), D ** -0.5, 0.09375, ((0, 8), (1, 4))),
        "w_out": scatter_about(arg_keys[7], (D, D), D ** -0.5, 0.09375, ((0, 4), (1, 8))),
    }


norm_eps = 1e-05
rope_theta = 500000.0

def rotate(heads_in, positions):
    half = heads_in.shape[-1] // 2
    freq = rope_theta ** (-2.0 * jnp.arange(half, dtype=jnp.float32) / heads_in.shape[-1])
    angle = positions.astype(jnp.float32)[:, None] * freq[None, :]
    cosine = jnp.cos(angle)[:, None, :]
    sine = jnp.sin(angle)[:, None, :]
    first = heads_in[..., :half]
    second = heads_in[..., half:]
    return jnp.concatenate([first * cosine - second * sine, second * cosine + first * sine], axis=-1)

def attend(query_rot, key_rot, value_rows, length):
    row_count = query_rot.shape[0]
    block = min(512, row_count)
    positions = jnp.arange(row_count, dtype=jnp.int32)
    keys_wide = key_rot.astype(jnp.float32)
    values_wide = value_rows.astype(jnp.float32)

    def one_block(offset):
        queries = lax.dynamic_slice_in_dim(query_rot, offset, block, 0).astype(jnp.float32)
        scores = jnp.einsum('qhgd,khd->hgqk', queries, keys_wide) / jnp.sqrt(jnp.float32(HD))
        query_pos = offset + jnp.arange(block, dtype=jnp.int32)
        allowed = (positions[None, :] <= query_pos[:, None]) & (positions[None, :] < length)
        scores = jnp.where(allowed, scores, -1e+30)
        biggest = lax.optimization_barrier(jnp.max(scores, axis=-1, keepdims=True))
        expd = jnp.exp(scores - biggest)
        weights = (expd / lax.optimization_barrier(jnp.sum(expd, axis=-1, keepdims=True))).astype(jnp.bfloat16)
        result = jnp.einsum('hgqk,khd->qhgd', weights.astype(jnp.float32), values_wide)
        return result.astype(jnp.bfloat16)
    starts = jnp.arange(0, row_count, block, dtype=jnp.int32)
    outs = lax.map(one_block, starts)
    return outs.reshape(row_count, -1)

def layer_group(token_ids, length, embed_table, norm_gain, w_query, w_key, w_value, w_out):
    row_count = token_ids.shape[0]
    tokens_in = jnp.take(embed_table, token_ids, axis=1).T
    wide_in = tokens_in.astype(jnp.float32)
    scale = lax.rsqrt(lax.optimization_barrier(jnp.mean(wide_in * wide_in, axis=1, keepdims=True)) + norm_eps)
    normed = (wide_in * scale * norm_gain.astype(jnp.float32)[None, :]).astype(jnp.bfloat16)
    query = jnp.dot(normed, w_query, preferred_element_type=jnp.float32)
    key_raw = jnp.dot(normed, w_key, preferred_element_type=jnp.float32)
    value_raw = jnp.dot(normed, w_value, preferred_element_type=jnp.float32)
    positions = jnp.arange(row_count, dtype=jnp.int32)
    query_rot = rotate(query.reshape(row_count, HEADS, HD), positions).astype(jnp.bfloat16)
    key_rot = rotate(key_raw.reshape(row_count, KVH, HD), positions).astype(jnp.bfloat16)
    value_rows = value_raw.reshape(row_count, KVH, HD).astype(jnp.bfloat16)
    attended = attend(query_rot.reshape(row_count, KVH, HEADS // KVH, HD), key_rot, value_rows, length)
    blocks = N_TENSOR // TPG
    block_width = D // N_TENSOR
    attended_four = attended.reshape(row_count, blocks, TPG, block_width).astype(jnp.float32)
    out_four = w_out.reshape(blocks, TPG, block_width, D).astype(jnp.float32)
    parts = jnp.einsum('rkmw,kmwd->mrd', attended_four, out_four)
    parts = lax.optimization_barrier(parts.astype(jnp.bfloat16)).astype(jnp.float32)
    hidden = (wide_in + lax.optimization_barrier(jnp.sum(parts, axis=0))).astype(jnp.bfloat16)
    kv_width = KVH * HD // N_TENSOR

    def member_major(table_rows):
        shaped = table_rows.reshape(row_count, blocks, TPG, kv_width)
        return shaped.transpose(2, 0, 1, 3).reshape(TPG, row_count, blocks * kv_width)
    cache = jnp.stack([member_major(key_rot.reshape(row_count, KVH * HD)), member_major(value_rows.reshape(row_count, KVH * HD))], axis=1)
    return (hidden, cache)

def reference(prompt_ids, prompt_lengths, embed_table, norm_gain, w_query, w_key, w_value, w_out):
    grouped_ids = prompt_ids.reshape(GROUPS, PROMPT)

    def one_group(pair):
        return layer_group(pair[0], pair[1], embed_table, norm_gain, w_query, w_key, w_value, w_out)
    hidden, cache = lax.map(one_group, (grouped_ids, prompt_lengths))
    return (hidden.reshape(GROUPS * PROMPT, D), cache.reshape(GROUPS * TPG, 2, PROMPT, KVH * HD // TPG))
```

```python
import jax
import jax.numpy as jnp
from jax import lax
from jax.experimental import pallas as pl
from jax.experimental.pallas import tpu as pltpu
from jax.sharding import PartitionSpec as P

HEADS = 32
KVH = 8
HD = 128
TPG = 4


norm_eps = 1e-05
rope_theta = 500000.0


def swapped(block, axis, apart):
    count = lax.axis_size(axis)
    route = []
    for low in range(count):
        high = low | 1 << apart
        if high != low and high < count:
            route += [(low, high), (high, low)]
    return lax.ppermute(block, axis, route)


def for_sending(shard):

    def short(part):
        return part.astype(jnp.bfloat16) if part.dtype == jnp.float32 else part

    return jax.tree.map(short, shard)


def rotate(heads_in, positions):
    half = heads_in.shape[-1] // 2
    freq = rope_theta ** (-2.0 * jnp.arange(half, dtype=jnp.float32) / heads_in.shape[-1])
    angle = positions.astype(jnp.float32)[:, None] * freq[None, :]
    cosine = jnp.cos(angle)[:, None, :]
    sine = jnp.sin(angle)[:, None, :]
    first = heads_in[..., :half]
    second = heads_in[..., half:]
    return jnp.concatenate(
        [first * cosine - second * sine, second * cosine + first * sine], axis=-1
    )


def attend(query_rot, key_rot, value_rows, length):
    row_count = query_rot.shape[0]
    block = min(512, row_count)
    positions = jnp.arange(row_count, dtype=jnp.int32)

    def one_block(offset):
        scores = jnp.einsum(
            "qhgd,khd->hgqk", query_rot, key_rot, preferred_element_type=jnp.float32
        ) / jnp.sqrt(jnp.float32(HD))
        query_pos = offset + jnp.arange(block, dtype=jnp.int32)
        allowed = (positions[None, :] <= query_pos[:, None]) & (positions[None, :] < length)
        scores = jnp.where(allowed, scores, -1e30)
        biggest = jnp.max(scores, axis=-1, keepdims=True)
        expd = jnp.exp(scores - biggest)
        weights = (expd / jnp.sum(expd, axis=-1, keepdims=True)).astype(jnp.bfloat16)
        result = jnp.einsum(
            "hgqk,khd->qhgd", weights, value_rows, preferred_element_type=jnp.float32
        )
        return result.astype(jnp.bfloat16)

    starts = jnp.arange(0, row_count, block, dtype=jnp.int32)
    outs = lax.map(one_block, starts)
    return outs.reshape(row_count, -1)


def ordered_pair(mine, theirs, bit_index, axis=0):
    upper_half = lax.axis_index("tensor") >> bit_index & 1 == 1
    first_half = jnp.where(upper_half, theirs, mine)
    second_half = jnp.where(upper_half, mine, theirs)
    return jnp.concatenate([first_half, second_half], axis=axis)


def collect_blocks(shard, swapper):
    stacked = shard[None]
    levels = lax.axis_size("tensor").bit_length() - 1
    for bit_index in range(TPG.bit_length() - 1, levels):
        stacked = ordered_pair(stacked, swapper(stacked, bit_index), bit_index)
    return stacked


def gather_in_group(own_part):
    bits = range(TPG.bit_length() - 1)
    width = own_part.shape[1] // len(bits)
    parts = [own_part[:, i * width : (i + 1) * width] for i in bits]
    axes = (1,) * len(bits)
    parts = [part.reshape(axes + part.shape) for part in parts]
    for step in bits:
        parts = [
            ordered_pair(
                part,
                swapped(part, "tensor", (i + step) % len(bits)),
                (i + step) % len(bits),
                len(bits) - 1 - (i + step) % len(bits),
            )
            for i, part in enumerate(parts)
        ]
    return jnp.concatenate([part.reshape(-1, width) for part in parts], axis=1)


def scatter_in_group(partial_sum):
    bits = range(TPG.bit_length() - 1)
    width = partial_sum.shape[1] // len(bits)
    rows = partial_sum.shape[0] // TPG
    shape = (2,) * len(bits) + (rows, width)
    parts = [partial_sum[:, i * width : (i + 1) * width].reshape(shape) for i in bits]
    for step in bits:
        moved = []
        for i, part in enumerate(parts):
            bit_index = (len(bits) - 1 - i - step) % len(bits)
            axis = len(bits) - 1 - bit_index
            lower = lax.slice_in_dim(part, 0, 1, axis=axis).astype(jnp.bfloat16)
            upper = lax.slice_in_dim(part, 1, 2, axis=axis).astype(jnp.bfloat16)
            upper_half = lax.axis_index("tensor") >> bit_index & 1 == 1
            kept = jnp.where(upper_half, upper, lower)
            given = jnp.where(upper_half, lower, upper)
            arrived = swapped(given, "tensor", bit_index)
            moved.append(kept.astype(jnp.float32) + arrived.astype(jnp.float32))
        parts = moved
    return jnp.concatenate([part.reshape(rows, width) for part in parts], axis=1)


def rms_normed(tokens_in, norm_gain):
    wide_in = tokens_in.astype(jnp.float32)
    scale = lax.rsqrt(jnp.mean(wide_in * wide_in, axis=1, keepdims=True) + norm_eps)
    return (wide_in * scale * norm_gain[None, :]).astype(jnp.bfloat16)


LANES = 128
PIECES = 6


def lookup_kernel(ids_ref, table_ref, out_ref, held, sems):
    columns, vocab = table_ref.shape
    tiles = vocab // LANES
    edges = [i * tiles // PIECES * LANES for i in range(PIECES + 1)]
    copies = [
        pltpu.make_async_copy(
            table_ref.at[:, low:high], held.at[:, low:high], sems.at[i]
        )
        for i, (low, high) in enumerate(zip(edges[:-1], edges[1:]))
    ]
    for copy in copies:
        copy.start()
    for copy in copies:
        copy.wait()
    lane = lax.broadcasted_iota(jnp.int32, (columns, LANES), 1)

    def block(index, carry):
        first = pl.multiple_of(index * LANES, LANES)

        def one(j, total):
            token = ids_ref[first + j]
            start = pl.multiple_of((token >> 7) * LANES, LANES)
            tile = held[:, pl.ds(start, LANES)].astype(jnp.float32)
            turned = pltpu.roll(tile, (j - token) & (LANES - 1), 1)
            return jnp.where(lane == j, turned, total)

        total = lax.fori_loop(
            0, LANES, one, jnp.zeros((columns, LANES), jnp.float32), unroll=8
        )
        out_ref[pl.ds(first, LANES), :] = total.T.astype(out_ref.dtype)
        return carry

    lax.fori_loop(0, out_ref.shape[0] // LANES, block, 0)


def lookup_rows(embed_table, token_ids):
    columns = embed_table.shape[0]
    return pl.pallas_call(
        lookup_kernel,
        out_shape=jax.ShapeDtypeStruct((token_ids.shape[0], columns), embed_table.dtype),
        in_specs=[
            pl.BlockSpec(memory_space=pltpu.SMEM),
            pl.BlockSpec(memory_space=pl.ANY),
        ],
        out_specs=pl.BlockSpec(memory_space=pltpu.VMEM),
        scratch_shapes=[
            pltpu.VMEM(embed_table.shape, embed_table.dtype),
            pltpu.SemaphoreType.DMA((PIECES,)),
        ],
        compiler_params=pltpu.CompilerParams(vmem_limit_bytes=48 << 20),
        cost_estimate=pl.CostEstimate(
            flops=0, bytes_accessed=2 * embed_table.size, transcendentals=0
        ),
    )(token_ids, embed_table)


def shards(prompt_ids, prompt_lengths, embed_table, norm_gain, w_query, w_key, w_value, w_out):
    quarter = prompt_ids.shape[0]
    row_count = quarter * TPG
    devices = lax.axis_size(("dp", "tensor"))
    columns = embed_table.shape[0]
    model_width = columns * devices
    group_index = (
        lax.axis_index("dp") * (lax.axis_size("tensor") // TPG) + lax.axis_index("tensor") // TPG
    )
    length = lax.dynamic_slice_in_dim(prompt_lengths, group_index, 1, 0)[0]
    all_ids = lax.all_gather(prompt_ids, ("dp", "tensor"), axis=0, tiled=True)
    picked = lookup_rows(embed_table, all_ids)
    outgoing = picked.reshape(devices, quarter, columns)
    arrived = lax.all_to_all(outgoing, ("dp", "tensor"), split_axis=0, concat_axis=2, tiled=True)
    own_rows = arrived.reshape(quarter, model_width)
    normed = gather_in_group(rms_normed(own_rows, norm_gain))
    query_width = w_query.shape[1]
    key_width = w_key.shape[1]
    packed = jnp.concatenate([w_query, w_key, w_value], axis=1)
    stacked = collect_blocks(
        packed,
        lambda values, bit_index: jax.tree.map(
            lambda part, own: part.astype(own.dtype),
            swapped(for_sending(values), "tensor", bit_index),
            values,
        ),
    )
    projected = jnp.einsum(
        "rd,kdc->rkc",
        normed,
        lax.all_gather(stacked, "dp", axis=1, tiled=True),
        preferred_element_type=jnp.float32,
    )
    blocks = projected.shape[1]
    local_heads = blocks * query_width // HD
    local_kv = blocks * key_width // HD
    positions = jnp.arange(row_count, dtype=jnp.int32)
    query = projected[:, :, :query_width].reshape(row_count, local_heads, HD)
    key_raw = projected[:, :, query_width : query_width + key_width].reshape(
        row_count, local_kv, HD
    )
    value_raw = projected[:, :, query_width + key_width :].reshape(row_count, local_kv, HD)
    query_rot = rotate(query, positions).astype(jnp.bfloat16)
    key_rot = rotate(key_raw, positions).astype(jnp.bfloat16)
    value_rows = value_raw.astype(jnp.bfloat16)
    cache = jnp.stack(
        [key_rot.reshape(row_count, local_kv * HD), value_rows.reshape(row_count, local_kv * HD)],
        axis=0,
    )[None]
    attended = attend(
        query_rot.reshape(row_count, local_kv, HEADS // KVH, HD), key_rot, value_rows, length
    )
    attended = attended.reshape(row_count, blocks, query_width)
    out_blocks = collect_blocks(
        w_out,
        lambda values, bit_index: jax.tree.map(
            lambda part, own: part.astype(own.dtype),
            swapped(for_sending(values), "tensor", bit_index),
            values,
        ),
    )
    partial_sum = jnp.einsum(
        "rkw,kwc->rc",
        attended,
        lax.all_gather(out_blocks, "dp", axis=2, tiled=True),
        preferred_element_type=jnp.float32,
    )
    running = scatter_in_group(partial_sum)
    hidden = (own_rows.astype(jnp.float32) + running).astype(jnp.bfloat16)
    return (hidden, cache)


def solution(mesh):
    in_specs = (
        P(("dp", "tensor")),
        P(),
        P(("dp", "tensor"), None),
        P(),
        P("dp", "tensor"),
        P("dp", "tensor"),
        P("dp", "tensor"),
        P("tensor", "dp"),
    )
    out_specs = (P(("dp", "tensor"), None), P(("dp", "tensor"), None, None, None))
    return jax.shard_map(shards, mesh=mesh, in_specs=in_specs, out_specs=out_specs, check_vma=False)
```

```python
import jax
import jax.numpy as jnp
from jax import lax
from jax.experimental import pallas as pl
from jax.experimental.pallas import tpu as pltpu
from jax.sharding import PartitionSpec as P

HEADS = 32
KVH = 8
HD = 128
TPG = 4


norm_eps = 1e-05
rope_theta = 500000.0


def swapped(block, axis, apart):
    count = lax.axis_size(axis)
    route = []
    for low in range(count):
        high = low | 1 << apart
        if high != low and high < count:
            route += [(low, high), (high, low)]
    return lax.ppermute(block, axis, route)


def for_sending(shard):

    def short(part):
        return part.astype(jnp.bfloat16) if part.dtype == jnp.float32 else part

    return jax.tree.map(short, shard)


def rotate(heads_in, positions):
    half = heads_in.shape[-1] // 2
    freq = rope_theta ** (-2.0 * jnp.arange(half, dtype=jnp.float32) / heads_in.shape[-1])
    angle = positions.astype(jnp.float32)[:, None] * freq[None, :]
    cosine = jnp.cos(angle)[:, None, :]
    sine = jnp.sin(angle)[:, None, :]
    first = heads_in[..., :half]
    second = heads_in[..., half:]
    return jnp.concatenate(
        [first * cosine - second * sine, second * cosine + first * sine], axis=-1
    )


def attend(query_rot, key_rot, value_rows, length):
    row_count = query_rot.shape[0]
    block = min(512, row_count)
    positions = jnp.arange(row_count, dtype=jnp.int32)

    def one_block(offset):
        scores = jnp.einsum(
            "qhgd,khd->hgqk", query_rot, key_rot, preferred_element_type=jnp.float32
        ) / jnp.sqrt(jnp.float32(HD))
        query_pos = offset + jnp.arange(block, dtype=jnp.int32)
        allowed = (positions[None, :] <= query_pos[:, None]) & (positions[None, :] < length)
        scores = jnp.where(allowed, scores, -1e30)
        biggest = jnp.max(scores, axis=-1, keepdims=True)
        expd = jnp.exp(scores - biggest)
        weights = (expd / jnp.sum(expd, axis=-1, keepdims=True)).astype(jnp.bfloat16)
        result = jnp.einsum(
            "hgqk,khd->qhgd", weights, value_rows, preferred_element_type=jnp.float32
        )
        return result.astype(jnp.bfloat16)

    starts = jnp.arange(0, row_count, block, dtype=jnp.int32)
    outs = lax.map(one_block, starts)
    return outs.reshape(row_count, -1)


def ordered_pair(mine, theirs, bit_index, axis=0):
    upper_half = lax.axis_index("tensor") >> bit_index & 1 == 1
    first_half = jnp.where(upper_half, theirs, mine)
    second_half = jnp.where(upper_half, mine, theirs)
    return jnp.concatenate([first_half, second_half], axis=axis)


def collect_blocks(shard, swapper):
    stacked = shard[None]
    levels = lax.axis_size("tensor").bit_length() - 1
    for bit_index in range(TPG.bit_length() - 1, levels):
        stacked = ordered_pair(stacked, swapper(stacked, bit_index), bit_index)
    return stacked


def gather_in_group(own_part):
    bits = range(TPG.bit_length() - 1)
    width = own_part.shape[1] // len(bits)
    parts = [own_part[:, i * width : (i + 1) * width] for i in bits]
    axes = (1,) * len(bits)
    parts = [part.reshape(axes + part.shape) for part in parts]
    for step in bits:
        parts = [
            ordered_pair(
                part,
                swapped(part, "tensor", (i + step) % len(bits)),
                (i + step) % len(bits),
                len(bits) - 1 - (i + step) % len(bits),
            )
            for i, part in enumerate(parts)
        ]
    return jnp.concatenate([part.reshape(-1, width) for part in parts], axis=1)


def scatter_in_group(partial_sum):
    bits = range(TPG.bit_length() - 1)
    width = partial_sum.shape[1] // len(bits)
    rows = partial_sum.shape[0] // TPG
    shape = (2,) * len(bits) + (rows, width)
    parts = [partial_sum[:, i * width : (i + 1) * width].reshape(shape) for i in bits]
    for step in bits:
        moved = []
        for i, part in enumerate(parts):
            bit_index = (len(bits) - 1 - i - step) % len(bits)
            axis = len(bits) - 1 - bit_index
            lower = lax.slice_in_dim(part, 0, 1, axis=axis).astype(jnp.bfloat16)
            upper = lax.slice_in_dim(part, 1, 2, axis=axis).astype(jnp.bfloat16)
            upper_half = lax.axis_index("tensor") >> bit_index & 1 == 1
            kept = jnp.where(upper_half, upper, lower)
            given = jnp.where(upper_half, lower, upper)
            arrived = swapped(given, "tensor", bit_index)
            moved.append(kept.astype(jnp.float32) + arrived.astype(jnp.float32))
        parts = moved
    return jnp.concatenate([part.reshape(rows, width) for part in parts], axis=1)


def rms_normed(tokens_in, norm_gain):
    wide_in = tokens_in.astype(jnp.float32)
    scale = lax.rsqrt(jnp.mean(wide_in * wide_in, axis=1, keepdims=True) + norm_eps)
    return (wide_in * scale * norm_gain[None, :]).astype(jnp.bfloat16)


OUT_PARTS = 2
LANES = 128
PIECES = 6


def lookup_kernel(ids_ref, table_ref, out_ref, held, sems):
    columns, vocab = table_ref.shape
    tiles = vocab // LANES
    edges = [i * tiles // PIECES * LANES for i in range(PIECES + 1)]
    copies = [
        pltpu.make_async_copy(
            table_ref.at[:, low:high], held.at[:, low:high], sems.at[i]
        )
        for i, (low, high) in enumerate(zip(edges[:-1], edges[1:]))
    ]
    for copy in copies:
        copy.start()
    for copy in copies:
        copy.wait()
    lane = lax.broadcasted_iota(jnp.int32, (columns, LANES), 1)

    def block(index, carry):
        first = pl.multiple_of(index * LANES, LANES)

        def one(j, total):
            token = ids_ref[first + j]
            start = pl.multiple_of((token >> 7) * LANES, LANES)
            tile = held[:, pl.ds(start, LANES)]
            turned = pltpu.roll(tile, (j - token) & (LANES - 1), 1)
            return jnp.where(lane == j, turned, total)

        total = lax.fori_loop(
            0, LANES, one, jnp.zeros((columns, LANES), out_ref.dtype), unroll=8
        )
        out_ref[pl.ds(first, LANES), :] = total.T
        return carry

    lax.fori_loop(0, out_ref.shape[0] // LANES, block, 0)


def lookup_rows(embed_table, token_ids):
    columns = embed_table.shape[0]
    return pl.pallas_call(
        lookup_kernel,
        out_shape=jax.ShapeDtypeStruct((token_ids.shape[0], columns), embed_table.dtype),
        in_specs=[
            pl.BlockSpec(memory_space=pltpu.SMEM),
            pl.BlockSpec(memory_space=pl.ANY),
        ],
        out_specs=pl.BlockSpec(memory_space=pltpu.VMEM),
        scratch_shapes=[
            pltpu.VMEM(embed_table.shape, embed_table.dtype),
            pltpu.SemaphoreType.DMA((PIECES,)),
        ],
        compiler_params=pltpu.CompilerParams(vmem_limit_bytes=48 << 20),
        cost_estimate=pl.CostEstimate(
            flops=0, bytes_accessed=2 * embed_table.size, transcendentals=0
        ),
    )(token_ids, embed_table)


def shards(prompt_ids, prompt_lengths, embed_table, norm_gain, w_query, w_key, w_value, w_out):
    quarter = prompt_ids.shape[0]
    row_count = quarter * TPG
    devices = lax.axis_size(("dp", "tensor"))
    columns = embed_table.shape[0]
    model_width = columns * devices
    group_index = (
        lax.axis_index("dp") * (lax.axis_size("tensor") // TPG) + lax.axis_index("tensor") // TPG
    )
    length = lax.dynamic_slice_in_dim(prompt_lengths, group_index, 1, 0)[0]
    all_ids = lax.all_gather(prompt_ids, ("dp", "tensor"), axis=0, tiled=True)
    all_ids, w_query, w_out = lax.optimization_barrier((all_ids, w_query, w_out))
    picked = lookup_rows(embed_table, all_ids)
    outgoing = picked.reshape(devices, quarter, columns)
    arrived = lax.all_to_all(outgoing, ("dp", "tensor"), split_axis=0, concat_axis=2, tiled=True)
    own_rows = arrived.reshape(quarter, model_width)
    normed = gather_in_group(rms_normed(own_rows, norm_gain))
    query_width = w_query.shape[1]
    key_width = w_key.shape[1]
    packed = jnp.concatenate([w_query, w_key, w_value], axis=1)
    stacked = collect_blocks(
        packed,
        lambda values, bit_index: jax.tree.map(
            lambda part, own: part.astype(own.dtype),
            swapped(for_sending(values), "tensor", bit_index),
            values,
        ),
    )
    projected = jnp.einsum(
        "rd,kdc->rkc",
        normed,
        lax.all_gather(stacked, "dp", axis=1, tiled=True),
        preferred_element_type=jnp.float32,
    )
    blocks = projected.shape[1]
    local_heads = blocks * query_width // HD
    local_kv = blocks * key_width // HD
    positions = jnp.arange(row_count, dtype=jnp.int32)
    query = projected[:, :, :query_width].reshape(row_count, local_heads, HD)
    key_raw = projected[:, :, query_width : query_width + key_width].reshape(
        row_count, local_kv, HD
    )
    value_raw = projected[:, :, query_width + key_width :].reshape(row_count, local_kv, HD)
    query_rot = rotate(query, positions).astype(jnp.bfloat16)
    key_rot = rotate(key_raw, positions).astype(jnp.bfloat16)
    value_rows = value_raw.astype(jnp.bfloat16)
    cache = jnp.stack(
        [key_rot.reshape(row_count, local_kv * HD), value_rows.reshape(row_count, local_kv * HD)],
        axis=0,
    )[None]
    attended = attend(
        query_rot.reshape(row_count, local_kv, HEADS // KVH, HD), key_rot, value_rows, length
    )
    attended = attended.reshape(row_count, blocks, query_width)
    out_blocks = collect_blocks(
        w_out,
        lambda values, bit_index: jax.tree.map(
            lambda part, own: part.astype(own.dtype),
            swapped(for_sending(values), "tensor", bit_index),
            values,
        ),
    )
    width = out_blocks.shape[2] // OUT_PARTS
    reduced = []
    for i in range(OUT_PARTS):
        piece = out_blocks[:, :, i * width : (i + 1) * width]
        partial_sum = jnp.einsum(
            "rkw,kwc->rc",
            attended,
            lax.all_gather(piece, "dp", axis=2, tiled=True),
            preferred_element_type=jnp.float32,
        )
        own_sum = scatter_in_group(partial_sum).reshape(quarter, -1, width)
        attended, own_sum = lax.optimization_barrier((attended, own_sum))
        reduced.append(own_sum)
    running = jnp.concatenate(reduced, axis=2).reshape(quarter, model_width)
    hidden = (own_rows.astype(jnp.float32) + running).astype(jnp.bfloat16)
    return (hidden, cache)


def solution(mesh):
    in_specs = (
        P(("dp", "tensor")),
        P(),
        P(("dp", "tensor"), None),
        P(),
        P("dp", "tensor"),
        P("dp", "tensor"),
        P("dp", "tensor"),
        P("tensor", "dp"),
    )
    out_specs = (P(("dp", "tensor"), None), P(("dp", "tensor"), None, None, None))
    return jax.shard_map(shards, mesh=mesh, in_specs=in_specs, out_specs=out_specs, check_vma=False)
```
